32 devices in a mesh: dp: 4 (over z), expert: 8 (over y, x, core).
Axes of the slice: x: 2, y: 2, z: 4, core: 2. Of those that a mesh axis runs over, the one named last changes fastest.
Arguments:
- tokens: bfloat16 [2048, 2048], P(('dp', 'expert')), may hold values from -6 to 6
- norm_gain: bfloat16 [2048], replicated, may hold values from 0.099609375 to 1.8984375
- router_weight: bfloat16 [2048, 8], replicated, may hold values from -0.125 to 0.125
- gate_weight: bfloat16 [8, 2048, 5120], P('expert', None, 'dp'), may hold values from -0.125 to 0.125
- up_weight: bfloat16 [8, 2048, 5120], P('expert', None, 'dp'), may hold values from -0.125 to 0.125
- down_weight: bfloat16 [8, 5120, 2048], P('expert', 'dp'), may hold values from -0.078125 to 0.078125
- expert_picks: int32 [4, 8, 128], P('dp'), may hold values from 0 to 511, as said below
- final_gain: bfloat16 [2048], replicated, may hold values from 0.099609375 to 1.8984375
- kv_weight: bfloat16 [2048, 8, 6, 2, 64], P(None, 'expert'), may hold values from -0.125 to 0.125
Outputs:
- moe_out: bfloat16 [2048, 2048], P(('dp', 'expert'))
- kv_cache: bfloat16 [2048, 8, 6, 2, 64], P('dp', 'expert')
The draws below stay inside these ranges and needn't reach their ends.
Inputs may be any that keep to these rules, and one draw needn't show every extreme that they name: `expert_picks`: for each group and expert, 128 different positions in the group. Of the 64 tokens of one device (positions s * 64 to (s + 1) * 64 - 1) one expert picks at most 32, and for every group and expert some device's tokens are picked exactly 32 times.
All inputs are finite; a program needn't handle non-finite values.
Results may differ from the reference program's by a relative error of at most 0.013.
Values may be sent and summed in bfloat16 or wider, within the bound.
A program may use at most 128 MiB of HBM per device.

```python
import jax
import jax.numpy as jnp
from jax import lax

D = 2048
FF = 5120
DK = 64
TOK_DEV = 64
LAYERS = 6
EXPERTS = 8
HEADS = 8
TOKENS = 2048
CAP = 128
MOST = 32
N_DP = 4
N_EXPERT = 8


def one_expert_picks(sub_key):
    key_full, key_slot, key_perm, key_order = jax.random.split(sub_key, 4)
    full_shard = jax.random.randint(key_full, (), 0, N_EXPERT)
    scores = jax.random.permutation(key_slot, N_EXPERT * MOST).astype(jnp.int32)
    shard_of = jnp.arange(N_EXPERT * MOST, dtype=jnp.int32) // MOST
    scores = jnp.where(shard_of == full_shard, scores - N_EXPERT * MOST, scores)
    chosen = jnp.argsort(scores, stable=True)[:CAP].astype(jnp.int32)
    shard_pos = chosen // MOST
    within = chosen % MOST
    shard_perms = jax.vmap(lambda perm_key: jax.random.permutation(perm_key, TOK_DEV))(jax.random.split(key_perm, N_EXPERT))
    token_pos = shard_pos * TOK_DEV + shard_perms[shard_pos, within].astype(jnp.int32)
    pick_order = jax.random.permutation(key_order, CAP)
    return token_pos[pick_order].astype(jnp.int32)


def draw_expert_picks(key, part):
    base = jax.random.fold_in(key, 7)
    keys = jax.random.split(base, N_DP * EXPERTS)
    all_picks = jax.vmap(one_expert_picks)(keys)
    return all_picks.reshape(N_DP, EXPERTS, CAP).astype(jnp.int32)


def levels(own_key, shape, shards, smallest, high):
    def one(axis_at, parts):
        draws = jax.random.uniform(jax.random.fold_in(jax.random.fold_in(own_key, 6), axis_at), (parts,), jnp.float32, smallest / len(shards), high / len(shards))
        return jnp.repeat(jnp.exp(draws), shape[axis_at] // parts).reshape((-1,) + (1,) * (len(shape) - axis_at - 1))

    level = one(*shards[0])
    for cut in shards[1:]:
        level = level * one(*cut)
    return level


def gaussian(key, dims, scale, bound, cuts=(), kind=jnp.bfloat16):
    level = levels(key, dims, cuts, -0.22, 0.18) if cuts else 1.0
    entries = jax.random.normal(key, dims, jnp.float32) * scale * level
    return jnp.minimum(jnp.maximum(entries, -bound), bound).astype(kind)


def setup_inputs(seed: int = 0) -> dict:
    key_list = jax.random.split(jax.random.key(seed), 10)
    tokens = gaussian(key_list[0], (TOKENS, D), 1.0, 6.0, ((0, 32),))
    norm_gain = jnp.clip(1.0 + 0.18 * jax.random.normal(key_list[1], (D,), jnp.float32), 0.099609375, 1.8984375).astype(jnp.bfloat16)
    router_weight = gaussian(key_list[2], (D, EXPERTS), D ** -0.5, 0.125)
    gate_weight = gaussian(key_list[3], (EXPERTS, D, FF), D ** -0.5, 0.125, ((0, 8), (2, 4)))
    up_weight = gaussian(key_list[4], (EXPERTS, D, FF), D ** -0.5, 0.125, ((0, 8), (2, 4)))
    down_weight = gaussian(key_list[5], (EXPERTS, FF, D), FF ** -0.5, 0.078125, ((0, 8), (1, 4)))
    expert_picks = draw_expert_picks(jax.random.fold_in(key_list[9], 71), 0)
    final_gain = jnp.clip(1.0 + 0.18 * jax.random.normal(key_list[7], (D,), jnp.float32), 0.099609375, 1.8984375).astype(jnp.bfloat16)
    kv_weight = gaussian(key_list[8], (D, HEADS, LAYERS, 2, DK), D ** -0.5, 0.125, ((1, 8),))
    return {"tokens": tokens, "norm_gain": norm_gain, "router_weight": router_weight, "gate_weight": gate_weight, "up_weight": up_weight, "down_weight": down_weight, "expert_picks": expert_picks, "final_gain": final_gain, "kv_weight": kv_weight}


def normalize(values, gain):
    return values * lax.rsqrt(lax.optimization_barrier(jnp.mean(values * values, axis=-1, keepdims=True)) + 1e-06) * gain.astype(jnp.float32)

def reference(tokens, norm_gain, router_weight, gate_weight, up_weight, down_weight, expert_picks, final_gain, kv_weight):
    wide_tokens = tokens.astype(jnp.float32)
    normed = normalize(wide_tokens, norm_gain).astype(jnp.bfloat16)
    gate_probs = jax.nn.sigmoid(jnp.dot(normed, router_weight, preferred_element_type=jnp.float32))
    group_start = jnp.arange(N_DP, dtype=jnp.int32)[:, None, None] * (TOK_DEV * N_EXPERT)
    all_rows = jnp.transpose(group_start + expert_picks, (1, 0, 2)).reshape(EXPERTS, -1).astype(jnp.int32)
    block_width = FF // N_DP

    def one_expert(expert):
        row_index = lax.dynamic_index_in_dim(all_rows, expert, 0, keepdims=False)
        inputs = normed[row_index]
        gate_act = jnp.dot(inputs, gate_weight[expert], preferred_element_type=jnp.float32)
        up_act = jnp.dot(inputs, up_weight[expert], preferred_element_type=jnp.float32)
        hidden = (jax.nn.gelu(gate_act, approximate=True) * up_act).astype(jnp.bfloat16)
        down_here = down_weight[expert]
        total = jnp.zeros((hidden.shape[0], D), jnp.float32)
        for block in range(N_DP):
            partial_sum = jnp.dot(hidden[:, block * block_width:(block + 1) * block_width], down_here[block * block_width:(block + 1) * block_width], preferred_element_type=jnp.float32).astype(jnp.bfloat16)
            partial_sum = lax.optimization_barrier(partial_sum)
            total = total + partial_sum.astype(jnp.float32)
        result = total.astype(jnp.bfloat16)
        weight = gate_probs[row_index, expert]
        return result.astype(jnp.float32) * weight[:, None]
    contributions = lax.map(one_expert, jnp.arange(EXPERTS, dtype=jnp.int32))
    combined = jnp.zeros((TOKENS, D), jnp.float32).at[all_rows.reshape(-1)].add(contributions.reshape(-1, D))
    moe_out = (wide_tokens + combined).astype(jnp.bfloat16)
    encoded = normalize(moe_out.astype(jnp.float32), final_gain).astype(jnp.bfloat16)
    projected = jnp.dot(encoded, kv_weight.reshape(D, -1), preferred_element_type=jnp.float32).astype(jnp.bfloat16)
    kv_cache = projected.reshape(TOKENS, HEADS, LAYERS, 2, DK)
    return (moe_out, kv_cache)
```

```python
import functools
import math

import jax
import jax.numpy as jnp
from jax import lax
from jax.experimental import pallas as pl
from jax.experimental.pallas import tpu as pltpu
from jax.sharding import PartitionSpec as P

MESH = pl.DeviceIdType.MESH
F32 = jnp.float32
BF16 = jnp.bfloat16


def plane_slots(side_a, side_b):
    return (side_a - 1) + (side_b - 1) + 1 + (side_a - 1) * (side_b - 1) + side_a * side_b - 1


def kernel(
    n, experts, side_a, side_b, ag_chunks, rs_chunks, lag, keep_map,
    tokens_hbm, gain_hbm, router_hbm, gate_hbm, up_hbm, down_hbm, picks_hbm, final_gain_hbm, kv_hbm,
    moe_out, kv_out,
    gate_w, up_w, down_w, kv_w, tokens_all, gathered, normed, hidden, part, sums, returned,
    gain16, final16, gain, final_gain, router, picks, pick_map, out_map, prob, squares, kv_acc, kv_stage,
    load_sem, ag_send, ag_recv, z_send, z_recv, rs_send, rs_recv, eo_send, eo_recv, out_sem,
):
    p = lax.axis_index("dp")
    me = lax.axis_index("expert")
    cap = picks.shape[1]
    group, width = tokens_all.shape
    rows = group // experts
    ff = gate_w.shape[1]
    heads = kv_acc.shape[0]
    core = lax.rem(me, 2)
    chip = lax.div(me, 2)
    row_at = lax.div(chip, side_b)
    col_at = lax.rem(chip, side_b)
    partner = chip * 2 + (1 - core)

    def span(index, size):
        return pl.ds(pl.multiple_of(index * size, size), size)

    own = span(me, rows)
    loads = [
        pltpu.make_async_copy(src, dst, load_sem.at[i])
        for i, (src, dst) in enumerate((
            (tokens_hbm, tokens_all.at[own]),
            (picks_hbm, picks),
            (gain_hbm, gain16),
            (final_gain_hbm, final16),
            (router_hbm, router),
            (gate_hbm.at[0], gate_w),
            (up_hbm.at[0], up_w),
            (down_hbm.at[0], down_w),
            (kv_hbm, kv_w),
        ))
    ]
    for load in loads:
        load.start()

    def place(a, b):
        return (lax.rem(a + side_a, side_a) * side_b + lax.rem(b + side_b, side_b)) * 2 + core

    square = side_a == side_b

    def peer(i, j, c):
        straight = place(row_at + j, col_at + i)
        if not square:
            return straight
        return jnp.where(lax.rem(c, 2) == 0, straight, place(row_at + i, col_at + j))

    barrier = pltpu.get_barrier_semaphore()

    def greet(target):
        pl.semaphore_signal(barrier, inc=1, device_id={"expert": target}, device_id_type=MESH)

    for i in range(1, side_b):
        greet(place(row_at, col_at + i))
    for j in range(1, side_a):
        greet(place(row_at + j, col_at))
    greet(partner)

    @pl.when(p > 0)
    def _():
        pl.semaphore_signal(barrier, inc=1, device_id={"dp": p - 1}, device_id_type=MESH)

    @pl.when(p < n - 1)
    def _():
        pl.semaphore_signal(barrier, inc=1, device_id={"dp": p + 1}, device_id_type=MESH)

    neighbours = jnp.where(p > 0, 1, 0) + jnp.where(p < n - 1, 1, 0)
    first_peers = range(1, side_b)
    second_peers = range(1, side_a)
    direct = side_a + side_b - 2

    class Plane:
        def __init__(self, full, unit, tile, send, recv):
            self.full, self.unit, self.tile, self.send, self.recv = full, unit, tile, send, recv

        def copy(self, c, source, target, slot):
            where = self.full.at[span(source, self.unit), span(c, self.tile)]
            return pltpu.make_async_remote_copy(
                src_ref=where,
                dst_ref=where,
                send_sem=self.send.at[slot, c],
                recv_sem=self.recv.at[source, c],
                device_id={"expert": target},
                device_id_type=MESH,
            )

        def start(self, c):
            for i in first_peers:
                self.copy(c, me, peer(i, 0, c), i - 1).start()
            for j in second_peers:
                self.copy(c, me, peer(0, j, c), side_b - 1 + j - 1).start()
            self.copy(c, me, partner, direct).start()

        def across(self, c, i, j):
            source = peer(-i, -j, c)
            slot = direct + 1 + (side_a - 1) * (side_b - 1) + i * side_a + j - 1
            piece = self.copy(c, source, partner, slot)
            piece.start()

        def relay(self, c):
            for i in first_peers:
                source = peer(-i, 0, c)
                self.copy(c, source, partner, 0).wait_recv()
                for j in second_peers:
                    slot = direct + 1 + (i - 1) * (side_a - 1) + j - 1
                    self.copy(c, source, peer(0, j, c), slot).start()
                self.across(c, i, 0)

        def collect(self, c):
            for j in second_peers:
                self.copy(c, peer(0, -j, c), partner, 0).wait_recv()
                self.across(c, 0, j)
            for i in first_peers:
                for j in second_peers:
                    self.copy(c, peer(-i, -j, c), partner, 0).wait_recv()
                    self.across(c, i, j)

        def arrive(self, c):
            for i in range(side_b):
                for j in range(side_a):
                    self.copy(c, peer(i, j, c) + 1 - 2 * core, partner, 0).wait_recv()

        def finish(self, c):
            for slot in range(plane_slots(side_a, side_b)):
                self.copy(c, me, partner, slot).wait_send()

    ag_tile = width // ag_chunks
    rs_tile = width // rs_chunks
    first = Plane(tokens_all, rows, ag_tile, ag_send, ag_recv)
    second = Plane(returned, cap, rs_tile, eo_send, eo_recv)

    loads[0].wait()
    pl.semaphore_wait(barrier, direct + 1 + neighbours)

    @pl.loop(0, ag_chunks)
    def _(c):
        first.start(c)

    for load in loads[1:5]:
        load.wait()

    lanes = 128
    for j in range(width // lanes):
        cols = pl.ds(j * lanes, lanes)
        gain[0:1, cols] = gain16[j:j + 1, :].astype(F32)
        final_gain[0:1, cols] = final16[j:j + 1, :].astype(F32)

    chosen = picks[pl.ds(me, 1), :].astype(F32)
    column = jnp.broadcast_to(chosen, (cap, cap)).T
    for j in range(group // cap):
        at = lax.broadcasted_iota(jnp.int32, (cap, cap), 1).astype(F32) + float(j * cap)
        pick_map[:, pl.ds(j * cap, cap)] = jnp.where(column == at, 1.0, 0.0).astype(BF16)

    def z_copy(g, c, way, target):
        piece = gathered.at[g, :, span(c, ag_tile)]
        return pltpu.make_async_remote_copy(
            src_ref=piece,
            dst_ref=piece,
            send_sem=z_send.at[way, g, c],
            recv_sem=z_recv.at[g, c],
            device_id={"dp": target},
            device_id_type=MESH,
        )

    def rs_copy(g, c, slot, target):
        return pltpu.make_async_remote_copy(
            src_ref=part.at[g, :, span(c, rs_tile)],
            dst_ref=sums.at[slot, :, span(c, rs_tile)],
            send_sem=rs_send.at[g, c],
            recv_sem=rs_recv.at[slot, c],
            device_id={"dp": target},
            device_id_type=MESH,
        )

    def rs_start(g, c):
        @pl.when(g < p)
        def _():
            rs_copy(g, c, g, p - 1).start()

        @pl.when(g > p)
        def _():
            rs_copy(g, c, jnp.where(g == p + 1, n, g), p + 1).start()

    @pl.loop(0, ag_chunks + 2)
    def _(s):
        @pl.when(s < ag_chunks)
        def _():
            first.relay(s)

        @pl.when((s >= 1) & (s <= ag_chunks))
        def _():
            first.collect(s - 1)

        @pl.when(s >= 2)
        def _():
            c = s - 2
            cols = span(c, ag_tile)
            first.arrive(c)
            gathered[p, :, cols] = jnp.dot(
                pick_map[...], tokens_all[:, cols], preferred_element_type=F32
            ).astype(BF16)

            @pl.when(p < n - 1)
            def _():
                z_copy(p, c, 0, p + 1).start()

            @pl.when(p > 0)
            def _():
                z_copy(p, c, 1, p - 1).start()

    map_rows = min(group, 256)

    def build_map(i):
        at = lax.broadcasted_iota(jnp.int32, (map_rows, cap), 0) + i * map_rows
        return jnp.concatenate(
            [jnp.where(picks[e:e + 1, :] == at, 1.0, 0.0).astype(BF16) for e in range(experts)], axis=1
        )

    if keep_map:
        @pl.loop(0, group // map_rows)
        def _(i):
            out_map[span(i, map_rows)] = build_map(i)

    kv_acc[...] = jnp.zeros_like(kv_acc)
    squares[...] = jnp.zeros_like(squares)

    @pl.when(p == 0)
    def _():
        sums[n] = jnp.zeros(sums.shape[1:], BF16)

    @pl.when(p == n - 1)
    def _():
        sums[p] = jnp.zeros(sums.shape[1:], BF16)

    for load in loads[5:]:
        load.wait()

    ff_tile = 256 if ff % 256 == 0 else 128
    norm_rows = 32

    def normalize(g):
        @pl.loop(0, cap // norm_rows)
        def _(i):
            piece = span(i, norm_rows)
            value = gathered[g, piece].astype(F32)
            scale = lax.rsqrt(jnp.mean(value * value, axis=-1, keepdims=True) + 1e-06)
            normed[piece] = (value * scale * gain[0:1, :]).astype(BF16)

    def compute(g):
        normalize(g)

        @pl.loop(0, ff // ff_tile)
        def _(i):
            cols = span(i, ff_tile)
            block = normed[...]
            gate = jnp.dot(block, gate_w[:, cols], preferred_element_type=F32)
            up = jnp.dot(block, up_w[:, cols], preferred_element_type=F32)
            hidden[:, cols] = (jax.nn.gelu(gate, approximate=True) * up).astype(BF16)

        @pl.loop(0, rs_chunks)
        def _(c):
            cols = span(c, rs_tile)
            part[g, :, cols] = jnp.dot(
                hidden[...], down_w[:, cols], preferred_element_type=F32
            ).astype(BF16)

            @pl.when(((g < p) & (p == n - 1)) | ((g > p) & (p == 0)))
            def _():
                rs_start(g, c)

    def forward(g, c):
        cols = span(c, rs_tile)
        rs_copy(g, c, g, p).wait_recv()
        part[g, :, cols] = (part[g, :, cols].astype(F32) + sums[g, :, cols].astype(F32)).astype(BF16)
        rs_start(g, c)

    leftmost = jnp.where(2 * p >= n - 1, 1, 0)
    closing = jnp.maximum(p, n - 1 - p)

    def flow(t, s):
        for turn in range(2):
            c = s - turn * lag
            to_left = leftmost if turn == 0 else 1 - leftmost
            g = jnp.where(to_left == 1, n - 1 - t, t)
            live = jnp.where(to_left == 1, (g < p) & (p < n - 1), (g > p) & (p > 0))

            @pl.when(live & (c >= 0) & (c < rs_chunks))
            def _():
                forward(g, c)

    def final(c):
        cols = span(c, rs_tile)

        @pl.when(p < n - 1)
        def _():
            rs_copy(p, c, p, p).wait_recv()

        @pl.when(p > 0)
        def _():
            rs_copy(p, c, n, p).wait_recv()

        value = (
            part[p, :, cols].astype(F32) + sums[p, :, cols].astype(F32) + sums[n, :, cols].astype(F32)
        )
        returned[span(me, cap), cols] = (value * prob[:, 0:1]).astype(BF16)
        second.start(c)

    compute(p)
    logits = lax.dot_general(
        normed[...], router[...], (((1,), (1,)), ((), ())), preferred_element_type=F32
    )
    mine = lax.broadcasted_iota(jnp.int32, logits.shape, 1) == me
    chance = jnp.sum(jnp.where(mine, jax.nn.sigmoid(logits), 0.0), axis=1, keepdims=True)
    prob[...] = jnp.broadcast_to(chance, prob.shape)

    def side_group(t, side):
        return p + t * (2 * side - 1)

    @pl.loop(1, n)
    def _(t):
        @pl.loop(0, ag_chunks)
        def _(c):
            for side in range(2):
                g = side_group(t, side)

                @pl.when((g >= 0) & (g < n))
                def _():
                    z_copy(g, c, 0, p).wait_recv()

                    onward = p + 1 - 2 * side

                    @pl.when((onward >= 0) & (onward < n))
                    def _():
                        z_copy(g, c, side, onward).start()

        @pl.loop(0, 2)
        def _(side):
            g = side_group(t, side)

            @pl.when((g >= 0) & (g < n))
            def _():
                compute(g)

        @pl.when(t < n - 1)
        def _():
            @pl.loop(0, rs_chunks + lag)
            def _(s):
                flow(t, s)

                @pl.when((t == closing) & (s >= lag))
                def _():
                    final(s - lag)

    @pl.loop(0, ag_chunks)
    def _(c):
        first.finish(c)

    def consume(c):
        cols = span(c, rs_tile)
        second.arrive(c)

        @pl.loop(0, group // map_rows)
        def _(i):
            piece = span(i, map_rows)
            chosen_map = out_map[piece] if keep_map else build_map(i)
            value = (
                tokens_all[piece, cols].astype(F32)
                + jnp.dot(chosen_map, returned[:, cols], preferred_element_type=F32)
            ).astype(BF16)
            tokens_all[piece, cols] = value
            wide = value.astype(F32)
            square_sum = wide * wide
            total = square_sum[:, 0:lanes]
            for j in range(1, rs_tile // lanes):
                total = total + square_sum[:, j * lanes:(j + 1) * lanes]
            squares[piece] += total
            scaled = (wide * final_gain[0:1, cols]).astype(BF16)
            kv_acc[:, piece] += lax.dot_general(
                kv_w[:, cols], scaled, (((1,), (1,)), ((), ())), preferred_element_type=F32
            )

    @pl.loop(0, rs_chunks + 3)
    def _(s):
        flow(n - 1, s)

        @pl.when((s < rs_chunks) & (closing == n - 1))
        def _():
            final(s)

        @pl.when((s >= 1) & (s <= rs_chunks))
        def _():
            second.relay(s - 1)

        @pl.when((s >= 2) & (s <= rs_chunks + 1))
        def _():
            second.collect(s - 2)

        @pl.when(s >= 3)
        def _():
            consume(s - 3)

    moe_store = pltpu.make_async_copy(tokens_all.at[own], moe_out, out_sem.at[0])
    moe_store.start()
    mean = jnp.sum(squares[...].T, axis=0, keepdims=True) * (1.0 / width)
    scale = lax.rsqrt(mean + 1e-06)
    out_rows = 128
    stores = []
    for i in range(heads // out_rows):
        piece = pl.ds(i * out_rows, out_rows)
        kv_stage[piece] = (kv_acc[piece] * scale).astype(BF16)
        store = pltpu.make_async_copy(kv_stage.at[piece], kv_out.at[piece], out_sem.at[1 + i])
        store.start()
        stores.append(store)

    @pl.loop(0, rs_chunks)
    def _(c):
        second.finish(c)

    @pl.loop(0, n)
    def _(g):
        @pl.loop(0, ag_chunks)
        def _(c):
            @pl.when((g <= p) & (p < n - 1))
            def _():
                z_copy(g, c, 0, p).wait_send()

            @pl.when((g >= p) & (p > 0))
            def _():
                z_copy(g, c, 1, p).wait_send()

        @pl.when(g != p)
        def _():
            @pl.loop(0, rs_chunks)
            def _(c):
                rs_copy(g, c, g, p).wait_send()

    moe_store.wait()
    for store in stores:
        store.wait()


def local(
    tokens,
    norm_gain,
    router_weight,
    gate_weight,
    up_weight,
    down_weight,
    expert_picks,
    final_gain,
    kv_weight,
):
    n = lax.axis_size("dp")
    experts = lax.axis_size("expert")
    rows, width = tokens.shape
    ff = gate_weight.shape[2]
    cap = expert_picks.shape[2]
    group = experts * rows
    chips = experts // 2
    side_a = max(d for d in range(1, math.isqrt(chips) + 1) if chips % d == 0)
    side_b = chips // side_a
    kv_matrix = kv_weight.reshape(width, -1).T
    heads = kv_matrix.shape[0]
    ag_chunks = 4
    rs_chunks = 4
    lag = 1
    keep_map = group * experts * cap * 2 <= 4 * 1024 * 1024
    dma = pltpu.SemaphoreType.DMA
    slots = plane_slots(side_a, side_b)
    hbm = pl.BlockSpec(memory_space=pl.ANY)
    moe_out, kv_rows = pl.pallas_call(
        functools.partial(kernel, n, experts, side_a, side_b, ag_chunks, rs_chunks, lag, keep_map),
        out_shape=(
            jax.ShapeDtypeStruct((rows, width), BF16),
            jax.ShapeDtypeStruct((heads, group), BF16),
        ),
        in_specs=[hbm] * 9,
        out_specs=(hbm, hbm),
        scratch_shapes=[
            pltpu.VMEM((width, ff), BF16),
            pltpu.VMEM((width, ff), BF16),
            pltpu.VMEM((ff, width), BF16),
            pltpu.VMEM((heads, width), BF16),
            pltpu.VMEM((group, width), BF16),
            pltpu.VMEM((n, cap, width), BF16),
            pltpu.VMEM((cap, width), BF16),
            pltpu.VMEM((cap, ff), BF16),
            pltpu.VMEM((n, cap, width), BF16),
            pltpu.VMEM((n + 1, cap, width), BF16),
            pltpu.VMEM((experts * cap, width), BF16),
            pltpu.VMEM((width // 128, 128), BF16),
            pltpu.VMEM((width // 128, 128), BF16),
            pltpu.VMEM((1, width), F32),
            pltpu.VMEM((1, width), F32),
            pltpu.VMEM((experts, width), BF16),
            pltpu.VMEM((experts, cap), jnp.int32),
            pltpu.VMEM((cap, group), BF16),
            pltpu.VMEM((group, experts * cap) if keep_map else (8, 128), BF16),
            pltpu.VMEM((cap, 128), F32),
            pltpu.VMEM((group, 128), F32),
            pltpu.VMEM((heads, group), F32),
            pltpu.VMEM((heads, group), BF16),
            dma((9,)),
            dma((slots, ag_chunks)),
            dma((experts, ag_chunks)),
            dma((2, n, ag_chunks)),
            dma((n, ag_chunks)),
            dma((n, rs_chunks)),
            dma((n + 1, rs_chunks)),
            dma((slots, rs_chunks)),
            dma((experts, rs_chunks)),
            dma((1 + heads // 128,)),
        ],
        compiler_params=pltpu.CompilerParams(
            collective_id=0, has_side_effects=True, vmem_limit_bytes=67043328
        ),
    )(
        tokens, norm_gain.reshape(-1, 128), router_weight.T, gate_weight, up_weight, down_weight,
        expert_picks[0], final_gain.reshape(-1, 128), kv_matrix,
    )
    kv_cache = kv_rows.T.reshape((group,) + kv_weight.shape[1:])
    return (moe_out, kv_cache)


def solution(mesh):
    in_specs = (
        P(("dp", "expert"), None),
        P(),
        P(),
        P("expert", None, "dp"),
        P("expert", None, "dp"),
        P("expert", "dp", None),
        P("dp", None, None),
        P(),
        P(None, "expert", None, None, None),
    )
    out_specs = (P(("dp", "expert"), None), P("dp", "expert", None, None, None))
    return jax.shard_map(local, mesh=mesh, in_specs=in_specs, out_specs=out_specs, check_vma=False)
```

```python
import functools
import math

import jax
import jax.numpy as jnp
from jax import lax
from jax.experimental import pallas as pl
from jax.experimental.pallas import tpu as pltpu
from jax.sharding import PartitionSpec as P

MESH = pl.DeviceIdType.MESH
F32 = jnp.float32
BF16 = jnp.bfloat16


def plane_slots(side_a, side_b):
    return (side_a - 1) + (side_b - 1) + 1 + (side_a - 1) * (side_b - 1) + side_a * side_b - 1


def kernel(
    n, experts, side_a, side_b, ag_chunks, rs_chunks, ahead, ag_routed, eo_routed, lag, depth, ff_steps, emit_group, keep_map,
    tokens_hbm, gain_hbm, router_hbm, gate_hbm, up_hbm, down_hbm, picks_hbm, final_gain_hbm, kv_hbm,
    moe_out, kv_out,
    gate_w, up_w, down_w, kv_w, tokens_all, gathered, feed, gate_acc, up_acc, row_squares, row_scale, hidden, part, sums, returned,
    gain16, final16, gain, final_gain, router, picks, pick_map, out_map, prob, squares, kv_acc, kv_stage,
    load_sem, ag_send, ag_recv, z_send, z_recv, rs_send, rs_recv, eo_send, eo_recv, out_sem,
):
    p = lax.axis_index("dp")
    me = lax.axis_index("expert")
    cap = picks.shape[1]
    group, width = tokens_all.shape
    rows = group // experts
    ff = gate_w.shape[1]
    heads = kv_acc.shape[0]
    core = lax.rem(me, 2)
    chip = lax.div(me, 2)
    row_at = lax.div(chip, side_b)
    col_at = lax.rem(chip, side_b)
    partner = chip * 2 + (1 - core)

    def span(index, size):
        return pl.ds(pl.multiple_of(index * size, size), size)

    own = span(me, rows)
    loads = [
        pltpu.make_async_copy(src, dst, load_sem.at[i])
        for i, (src, dst) in enumerate((
            (tokens_hbm, tokens_all.at[own]),
            (picks_hbm, picks),
            (gain_hbm, gain16),
            (final_gain_hbm, final16),
            (router_hbm, router),
            (gate_hbm.at[0], gate_w),
            (up_hbm.at[0], up_w),
            (down_hbm.at[0], down_w),
            (kv_hbm, kv_w),
        ))
    ]
    for load in loads:
        load.start()

    def place(a, b):
        return (lax.rem(a + side_a, side_a) * side_b + lax.rem(b + side_b, side_b)) * 2 + core

    square = side_a == side_b

    def peer(i, j, c):
        straight = place(row_at + j, col_at + i)
        if not square:
            return straight
        return jnp.where(lax.rem(c, 2) == 0, straight, place(row_at + i, col_at + j))

    barrier = pltpu.get_barrier_semaphore()

    def greet(target):
        pl.semaphore_signal(barrier, inc=1, device_id={"expert": target}, device_id_type=MESH)

    greeted = [
        (j, i) for j in range(side_a) for i in range(side_b)
        if (i > 0 or j > 0) and (i == 0 or j == 0 or ag_routed + eo_routed > 0)
    ]
    for j, i in greeted:
        greet(place(row_at + j, col_at + i))
    greet(partner)

    @pl.when(p > 0)
    def _():
        pl.semaphore_signal(barrier, inc=1, device_id={"dp": p - 1}, device_id_type=MESH)

    @pl.when(p < n - 1)
    def _():
        pl.semaphore_signal(barrier, inc=1, device_id={"dp": p + 1}, device_id_type=MESH)

    neighbours = jnp.where(p > 0, 1, 0) + jnp.where(p < n - 1, 1, 0)
    first_peers = range(1, side_b)
    second_peers = range(1, side_a)
    direct = side_a + side_b - 2

    class Plane:
        def __init__(self, full, unit, tile, send, recv, routed):
            self.full, self.unit, self.tile, self.send, self.recv = full, unit, tile, send, recv
            self.routed = routed

        def copy(self, c, source, target, slot):
            where = self.full.at[span(source, self.unit), span(c, self.tile)]
            return pltpu.make_async_remote_copy(
                src_ref=where,
                dst_ref=where,
                send_sem=self.send.at[slot, c],
                recv_sem=self.recv.at[source, c],
                device_id={"expert": target},
                device_id_type=MESH,
            )

        def start(self, c):
            for i in first_peers:
                self.copy(c, me, peer(i, 0, c), i - 1).start()
            for j in second_peers:
                self.copy(c, me, peer(0, j, c), side_b - 1 + j - 1).start()
            self.copy(c, me, partner, direct).start()

            @pl.when(self.routed(c))
            def _():
                for i in first_peers:
                    for j in second_peers:
                        self.copy(c, me, peer(i, j, c), direct + 1 + (i - 1) * (side_a - 1) + j - 1).start()

        def across(self, c, i, j):
            source = peer(-i, -j, c)
            slot = direct + 1 + (side_a - 1) * (side_b - 1) + i * side_a + j - 1
            piece = self.copy(c, source, partner, slot)
            piece.start()

        def relay(self, c):
            for i in first_peers:
                source = peer(-i, 0, c)
                self.copy(c, source, partner, 0).wait_recv()

                @pl.when(jnp.logical_not(self.routed(c)))
                def _():
                    for j in second_peers:
                        slot = direct + 1 + (i - 1) * (side_a - 1) + j - 1
                        self.copy(c, source, peer(0, j, c), slot).start()

                self.across(c, i, 0)

        def collect(self, c):
            for j in second_peers:
                self.copy(c, peer(0, -j, c), partner, 0).wait_recv()
                self.across(c, 0, j)
            for i in first_peers:
                for j in second_peers:
                    self.copy(c, peer(-i, -j, c), partner, 0).wait_recv()
                    self.across(c, i, j)

        def arrive(self, c):
            for i in range(side_b):
                for j in range(side_a):
                    self.copy(c, peer(i, j, c) + 1 - 2 * core, partner, 0).wait_recv()

        def finish(self, c):
            for slot in range(plane_slots(side_a, side_b)):
                self.copy(c, me, partner, slot).wait_send()

    ag_tile = width // ag_chunks
    rs_tile = width // rs_chunks
    first = Plane(tokens_all, rows, ag_tile, ag_send, ag_recv, lambda c: c < ag_routed)
    second = Plane(returned, cap, rs_tile, eo_send, eo_recv, lambda c: c >= rs_chunks - eo_routed)

    loads[0].wait()
    pl.semaphore_wait(barrier, len(greeted) + 1 + neighbours)

    for c in range(min(ahead, ag_chunks)):
        first.start(c)

    for load in loads[1:5]:
        load.wait()

    lanes = 128
    for j in range(width // lanes):
        cols = pl.ds(j * lanes, lanes)
        gain[0:1, cols] = gain16[j:j + 1, :].astype(F32)
        final_gain[0:1, cols] = final16[j:j + 1, :].astype(F32)

    chosen = picks[pl.ds(me, 1), :].astype(F32)
    column = jnp.broadcast_to(chosen, (cap, cap)).T
    for j in range(group // cap):
        at = lax.broadcasted_iota(jnp.int32, (cap, cap), 1).astype(F32) + float(j * cap)
        pick_map[:, pl.ds(j * cap, cap)] = jnp.where(column == at, 1.0, 0.0).astype(BF16)

    def z_copy(g, c, way, target):
        piece = gathered.at[g, :, span(c, ag_tile)]
        return pltpu.make_async_remote_copy(
            src_ref=piece,
            dst_ref=piece,
            send_sem=z_send.at[way, g, c],
            recv_sem=z_recv.at[g, c],
            device_id={"dp": target},
            device_id_type=MESH,
        )

    def rs_copy(g, c, slot, target):
        return pltpu.make_async_remote_copy(
            src_ref=part.at[g, :, span(c, rs_tile)],
            dst_ref=sums.at[slot, :, span(c, rs_tile)],
            send_sem=rs_send.at[g, c],
            recv_sem=rs_recv.at[slot, c],
            device_id={"dp": target},
            device_id_type=MESH,
        )

    def rs_start(g, c):
        @pl.when(g < p)
        def _():
            rs_copy(g, c, g, p - 1).start()

        @pl.when(g > p)
        def _():
            rs_copy(g, c, jnp.where(g == p + 1, n, g), p + 1).start()

    @pl.loop(0, ag_chunks + 2)
    def _(s):
        @pl.when(s < ag_chunks)
        def _():
            first.relay(s)

        @pl.when(s + ahead < ag_chunks)
        def _():
            first.start(s + ahead)

        @pl.when((s >= 1) & (s <= ag_chunks))
        def _():
            first.collect(s - 1)

        @pl.when(s >= 2)
        def _():
            c = s - 2
            cols = span(c, ag_tile)
            first.arrive(c)
            gathered[p, :, cols] = jnp.dot(
                pick_map[...], tokens_all[:, cols], preferred_element_type=F32
            ).astype(BF16)

            @pl.when(p < n - 1)
            def _():
                z_copy(p, c, 0, p + 1).start()

            @pl.when(p > 0)
            def _():
                z_copy(p, c, 1, p - 1).start()

    map_rows = min(group, 512) if keep_map else 256

    def build_map(i):
        at = lax.broadcasted_iota(jnp.int32, (map_rows, cap), 0) + i * map_rows
        return jnp.concatenate(
            [jnp.where(picks[e:e + 1, :] == at, 1.0, 0.0).astype(BF16) for e in range(experts)], axis=1
        )

    if keep_map:
        @pl.loop(0, group // map_rows)
        def _(i):
            out_map[span(i, map_rows)] = build_map(i)

    kv_acc[...] = jnp.zeros_like(kv_acc)
    squares[...] = jnp.zeros_like(squares)

    @pl.when(p == 0)
    def _():
        sums[n] = jnp.zeros(sums.shape[1:], BF16)

    @pl.when(p == n - 1)
    def _():
        sums[p] = jnp.zeros(sums.shape[1:], BF16)

    for load in loads[5:]:
        load.wait()

    ff_tile = ff // ff_steps

    def absorb(g, c, slot):
        cols = pl.ds(c * ag_tile, ag_tile)
        value = gathered[g, :, cols].astype(F32)
        squared = value * value
        total = squared[:, 0:lanes]
        for j in range(1, ag_tile // lanes):
            total = total + squared[:, j * lanes:(j + 1) * lanes]
        if c > 0:
            total = total + row_squares[slot]
        row_squares[slot] = total
        feed[...] = (value * gain[0:1, cols]).astype(BF16)
        closes = c == ag_chunks - 1
        if closes:
            row_scale[slot] = jnp.broadcast_to(
                lax.rsqrt(jnp.sum(total, axis=1, keepdims=True) * (1.0 / width) + 1e-06), total.shape
            )

        @pl.loop(0, ff // ff_tile)
        def _(i):
            tile = span(i, ff_tile)
            block = feed[...]
            gate = jnp.dot(block, gate_w[cols, tile], preferred_element_type=F32)
            up = jnp.dot(block, up_w[cols, tile], preferred_element_type=F32)
            if c > 0:
                gate = gate + gate_acc[slot, :, tile]
                up = up + up_acc[slot, :, tile]
            if closes:
                scale = row_scale[slot, :, 0:1]
                hidden[:, tile] = (jax.nn.gelu(gate * scale, approximate=True) * (up * scale)).astype(BF16)
            else:
                gate_acc[slot, :, tile] = gate
                up_acc[slot, :, tile] = up

    def emit(g):
        leads = ((g < p) & (p == n - 1)) | ((g > p) & (p == 0))
        wide = rs_tile * emit_group

        @pl.loop(0, rs_chunks // emit_group)
        def _(i):
            cols = span(i, wide)
            part[g, :, cols] = jnp.dot(
                hidden[...], down_w[:, cols], preferred_element_type=F32
            ).astype(BF16)

            @pl.when(leads)
            def _():
                for j in range(emit_group):
                    rs_start(g, i * emit_group + j)

    def forward(g, c):
        cols = span(c, rs_tile)
        rs_copy(g, c, g, p).wait_recv()
        part[g, :, cols] = (part[g, :, cols].astype(F32) + sums[g, :, cols].astype(F32)).astype(BF16)
        rs_start(g, c)

    leftmost = jnp.where(2 * p >= n - 1, 1, 0)
    closing = jnp.maximum(p, n - 1 - p)

    def flow(t, s):
        for turn in range(2):
            c = s - turn * lag
            to_left = leftmost if turn == 0 else 1 - leftmost
            g = jnp.where(to_left == 1, n - 1 - t, t)
            live = jnp.where(to_left == 1, (g < p) & (p < n - 1), (g > p) & (p > 0))

            @pl.when(live & (c >= 0) & (c < rs_chunks))
            def _():
                forward(g, c)

    def final(c):
        cols = span(c, rs_tile)

        @pl.when(p < n - 1)
        def _():
            rs_copy(p, c, p, p).wait_recv()

        @pl.when(p > 0)
        def _():
            rs_copy(p, c, n, p).wait_recv()

        value = (
            part[p, :, cols].astype(F32) + sums[p, :, cols].astype(F32) + sums[n, :, cols].astype(F32)
        )

        returned[span(me, cap), cols] = (value * prob[:, 0:1]).astype(BF16)
        second.start(c)

    logits = jnp.zeros((cap, experts), F32)
    for c in range(ag_chunks):
        absorb(p, c, 0)
        logits = logits + lax.dot_general(
            feed[...], router[:, pl.ds(c * ag_tile, ag_tile)], (((1,), (1,)), ((), ())), preferred_element_type=F32
        )
    emit(p)
    logits = logits * row_scale[0, :, 0:1]
    mine = lax.broadcasted_iota(jnp.int32, logits.shape, 1) == me
    chance = jnp.sum(jnp.where(mine, jax.nn.sigmoid(logits), 0.0), axis=1, keepdims=True)
    prob[...] = jnp.broadcast_to(chance, prob.shape)

    def side_group(t, side):
        return p + t * (2 * side - 1)

    @pl.loop(1, n)
    def _(t):
        for c in range(ag_chunks):
            for side in range(2):
                g = side_group(t, side)

                @pl.when((g >= 0) & (g < n))
                def _():
                    z_copy(g, c, 0, p).wait_recv()
                    onward = p + 1 - 2 * side

                    @pl.when((onward >= 0) & (onward < n))
                    def _():
                        z_copy(g, c, side, onward).start()

                    absorb(g, c, side)
                    if c == ag_chunks - 1:
                        emit(g)

        @pl.when(t < n - 1)
        def _():
            @pl.loop(0, rs_chunks + lag)
            def _(s):
                flow(t, s)

                @pl.when((t == closing) & (s >= lag))
                def _():
                    final(s - lag)

    @pl.loop(0, ag_chunks)
    def _(c):
        first.finish(c)

    def consume(c):
        cols = span(c, rs_tile)
        second.arrive(c)

        @pl.loop(0, group // map_rows)
        def _(i):
            piece = span(i, map_rows)
            chosen_map = out_map[piece] if keep_map else build_map(i)
            value = (
                tokens_all[piece, cols].astype(F32)
                + jnp.dot(chosen_map, returned[:, cols], preferred_element_type=F32)
            ).astype(BF16)
            tokens_all[piece, cols] = value
            wide = value.astype(F32)
            square_sum = wide * wide
            total = square_sum[:, 0:lanes]
            for j in range(1, rs_tile // lanes):
                total = total + square_sum[:, j * lanes:(j + 1) * lanes]
            squares[piece] += total
            scaled = (wide * final_gain[0:1, cols]).astype(BF16)
            kv_acc[:, piece] += lax.dot_general(
                kv_w[:, cols], scaled, (((1,), (1,)), ((), ())), preferred_element_type=F32
            )

    @pl.loop(0, rs_chunks + 3 * depth)
    def _(s):
        flow(n - 1, s)

        @pl.when((s < rs_chunks) & (closing == n - 1))
        def _():
            final(s)

        @pl.when((s >= depth) & (s < rs_chunks + depth))
        def _():
            second.relay(s - depth)

        @pl.when((s >= 2 * depth) & (s < rs_chunks + 2 * depth))
        def _():
            second.collect(s - 2 * depth)

        @pl.when(s >= 3 * depth)
        def _():
            consume(s - 3 * depth)

    moe_store = pltpu.make_async_copy(tokens_all.at[own], moe_out, out_sem.at[0])
    moe_store.start()
    mean = jnp.sum(squares[...].T, axis=0, keepdims=True) * (1.0 / width)
    scale = lax.rsqrt(mean + 1e-06)
    out_rows = 128
    stores = []
    for i in range(heads // out_rows):
        piece = pl.ds(i * out_rows, out_rows)
        kv_stage[piece] = (kv_acc[piece] * scale).astype(BF16)
        store = pltpu.make_async_copy(kv_stage.at[piece], kv_out.at[piece], out_sem.at[1 + i])
        store.start()
        stores.append(store)

    @pl.loop(0, rs_chunks)
    def _(c):
        second.finish(c)

    @pl.loop(0, n)
    def _(g):
        @pl.loop(0, ag_chunks)
        def _(c):
            @pl.when((g <= p) & (p < n - 1))
            def _():
                z_copy(g, c, 0, p).wait_send()

            @pl.when((g >= p) & (p > 0))
            def _():
                z_copy(g, c, 1, p).wait_send()

        @pl.when(g != p)
        def _():
            @pl.loop(0, rs_chunks)
            def _(c):
                rs_copy(g, c, g, p).wait_send()

    moe_store.wait()
    for store in stores:
        store.wait()


def local(
    tokens,
    norm_gain,
    router_weight,
    gate_weight,
    up_weight,
    down_weight,
    expert_picks,
    final_gain,
    kv_weight,
):
    n = lax.axis_size("dp")
    experts = lax.axis_size("expert")
    rows, width = tokens.shape
    ff = gate_weight.shape[2]
    cap = expert_picks.shape[2]
    group = experts * rows
    chips = experts // 2
    side_a = max(d for d in range(1, math.isqrt(chips) + 1) if chips % d == 0)
    side_b = chips // side_a
    kv_matrix = kv_weight.reshape(width, -1).T
    heads = kv_matrix.shape[0]
    ag_chunks = 4
    rs_chunks = 8
    ahead = 2
    ag_routed = 0
    eo_routed = 0
    lag = 2
    depth = 2
    ff_steps = 1
    emit_group = 4
    keep_map = group * experts * cap * 2 <= 4 * 1024 * 1024
    dma = pltpu.SemaphoreType.DMA
    slots = plane_slots(side_a, side_b)
    hbm = pl.BlockSpec(memory_space=pl.ANY)
    moe_out, kv_rows = pl.pallas_call(
        functools.partial(kernel, n, experts, side_a, side_b, ag_chunks, rs_chunks, ahead, ag_routed, eo_routed, lag, depth, ff_steps, emit_group, keep_map),
        out_shape=(
            jax.ShapeDtypeStruct((rows, width), BF16),
            jax.ShapeDtypeStruct((heads, group), BF16),
        ),
        in_specs=[hbm] * 9,
        out_specs=(hbm, hbm),
        scratch_shapes=[
            pltpu.VMEM((width, ff), BF16),
            pltpu.VMEM((width, ff), BF16),
            pltpu.VMEM((ff, width), BF16),
            pltpu.VMEM((heads, width), BF16),
            pltpu.VMEM((group, width), BF16),
            pltpu.VMEM((n, cap, width), BF16),
            pltpu.VMEM((cap, width // ag_chunks), BF16),
            pltpu.VMEM((2, cap, ff), F32),
            pltpu.VMEM((2, cap, ff), F32),
            pltpu.VMEM((2, cap, 128), F32),
            pltpu.VMEM((2, cap, 128), F32),
            pltpu.VMEM((cap, ff), BF16),
            pltpu.VMEM((n, cap, width), BF16),
            pltpu.VMEM((n + 1, cap, width), BF16),
            pltpu.VMEM((experts * cap, width), BF16),
            pltpu.VMEM((width // 128, 128), BF16),
            pltpu.VMEM((width // 128, 128), BF16),
            pltpu.VMEM((1, width), F32),
            pltpu.VMEM((1, width), F32),
            pltpu.VMEM((experts, width), BF16),
            pltpu.VMEM((experts, cap), jnp.int32),
            pltpu.VMEM((cap, group), BF16),
            pltpu.VMEM((group, experts * cap) if keep_map else (8, 128), BF16),
            pltpu.VMEM((cap, 128), F32),
            pltpu.VMEM((group, 128), F32),
            pltpu.VMEM((heads, group), F32),
            pltpu.VMEM((heads, group), BF16),
            dma((9,)),
            dma((slots, ag_chunks)),
            dma((experts, ag_chunks)),
            dma((2, n, ag_chunks)),
            dma((n, ag_chunks)),
            dma((n, rs_chunks)),
            dma((n + 1, rs_chunks)),
            dma((slots, rs_chunks)),
            dma((experts, rs_chunks)),
            dma((1 + heads // 128,)),
        ],
        compiler_params=pltpu.CompilerParams(
            collective_id=0, has_side_effects=True, vmem_limit_bytes=67043328
        ),
    )(
        tokens, norm_gain.reshape(-1, 128), router_weight.T, gate_weight, up_weight, down_weight,
        expert_picks[0], final_gain.reshape(-1, 128), kv_matrix,
    )
    kv_cache = kv_rows.T.reshape((group,) + kv_weight.shape[1:])
    return (moe_out, kv_cache)


def solution(mesh):
    in_specs = (
        P(("dp", "expert"), None),
        P(),
        P(),
        P("expert", None, "dp"),
        P("expert", None, "dp"),
        P("expert", "dp", None),
        P("dp", None, None),
        P(),
        P(None, "expert", None, None, None),
    )
    out_specs = (P(("dp", "expert"), None), P("dp", "expert", None, None, None))
    return jax.shard_map(local, mesh=mesh, in_specs=in_specs, out_specs=out_specs, check_vma=False)
```

```python
import functools
import math

import jax
import jax.numpy as jnp
from jax import lax
from jax.experimental import pallas as pl
from jax.experimental.pallas import tpu as pltpu
from jax.sharding import PartitionSpec as P

MESH = pl.DeviceIdType.MESH
F32 = jnp.float32
BF16 = jnp.bfloat16


def plane_slots(side_a, side_b):
    return (side_a - 1) + (side_b - 1) + 1 + (side_a - 1) * (side_b - 1) + side_a * side_b - 1


def kernel(
    n, experts, side_a, side_b, ag_chunks, rs_chunks, ahead, ag_routed, eo_routed, lag, depth, ff_steps, emit_group, keep_map,
    tokens_hbm, gain_hbm, router_hbm, gate_hbm, up_hbm, down_hbm, picks_hbm, final_gain_hbm, kv_hbm,
    moe_out, kv_out,
    gate_w, up_w, down_w, kv_w, tokens_all, gathered, feed, gate_acc, up_acc, row_squares, row_scale, hidden, part, sums, returned,
    gain16, final16, gain, final_gain, router, picks, pick_map, out_map, prob, squares, kv_acc, kv_stage,
    load_sem, ag_send, ag_recv, z_send, z_recv, rs_send, rs_recv, eo_send, eo_recv, out_sem,
):
    p = lax.axis_index("dp")
    me = lax.axis_index("expert")
    cap = picks.shape[1]
    group, width = tokens_all.shape
    rows = group // experts
    ff = gate_w.shape[1]
    heads = kv_acc.shape[0]
    core = lax.rem(me, 2)
    chip = lax.div(me, 2)
    row_at = lax.div(chip, side_b)
    col_at = lax.rem(chip, side_b)
    partner = chip * 2 + (1 - core)

    def span(index, size):
        return pl.ds(pl.multiple_of(index * size, size), size)

    own = span(me, rows)
    loads = [
        pltpu.make_async_copy(src, dst, load_sem.at[i])
        for i, (src, dst) in enumerate((
            (tokens_hbm, tokens_all.at[own]),
            (picks_hbm, picks),
            (gain_hbm, gain16),
            (final_gain_hbm, final16),
            (router_hbm, router),
            (gate_hbm.at[0], gate_w),
            (up_hbm.at[0], up_w),
            (down_hbm.at[0], down_w),
            (kv_hbm, kv_w),
        ))
    ]
    for load in loads:
        load.start()

    def place(a, b):
        return (lax.rem(a + side_a, side_a) * side_b + lax.rem(b + side_b, side_b)) * 2 + core

    square = side_a == side_b

    def peer(i, j, c):
        straight = place(row_at + j, col_at + i)
        if not square:
            return straight
        return jnp.where(lax.rem(c, 2) == 0, straight, place(row_at + i, col_at + j))

    barrier = pltpu.get_barrier_semaphore()

    def greet(target):
        pl.semaphore_signal(barrier, inc=1, device_id={"expert": target}, device_id_type=MESH)

    greeted = [
        (j, i) for j in range(side_a) for i in range(side_b)
        if (i > 0 or j > 0) and (i == 0 or j == 0 or ag_routed + eo_routed > 0)
    ]
    for j, i in greeted:
        greet(place(row_at + j, col_at + i))
    greet(partner)

    @pl.when(p > 0)
    def _():
        pl.semaphore_signal(barrier, inc=1, device_id={"dp": p - 1}, device_id_type=MESH)

    @pl.when(p < n - 1)
    def _():
        pl.semaphore_signal(barrier, inc=1, device_id={"dp": p + 1}, device_id_type=MESH)

    neighbours = jnp.where(p > 0, 1, 0) + jnp.where(p < n - 1, 1, 0)
    first_peers = range(1, side_b)
    second_peers = range(1, side_a)
    direct = side_a + side_b - 2

    class Plane:
        def __init__(self, full, unit, tile, send, recv, routed):
            self.full, self.unit, self.tile, self.send, self.recv = full, unit, tile, send, recv
            self.routed = routed

        def copy(self, c, source, target, slot):
            where = self.full.at[span(source, self.unit), span(c, self.tile)]
            return pltpu.make_async_remote_copy(
                src_ref=where,
                dst_ref=where,
                send_sem=self.send.at[slot, c],
                recv_sem=self.recv.at[source, c],
                device_id={"expert": target},
                device_id_type=MESH,
            )

        def start(self, c):
            for i in first_peers:
                self.copy(c, me, peer(i, 0, c), i - 1).start()
            for j in second_peers:
                self.copy(c, me, peer(0, j, c), side_b - 1 + j - 1).start()
            self.copy(c, me, partner, direct).start()

            @pl.when(self.routed(c))
            def _():
                for i in first_peers:
                    for j in second_peers:
                        self.copy(c, me, peer(i, j, c), direct + 1 + (i - 1) * (side_a - 1) + j - 1).start()

        def across(self, c, i, j):
            source = peer(-i, -j, c)
            slot = direct + 1 + (side_a - 1) * (side_b - 1) + i * side_a + j - 1
            piece = self.copy(c, source, partner, slot)
            piece.start()

        def relay(self, c):
            for i in first_peers:
                source = peer(-i, 0, c)
                self.copy(c, source, partner, 0).wait_recv()

                @pl.when(jnp.logical_not(self.routed(c)))
                def _():
                    for j in second_peers:
                        slot = direct + 1 + (i - 1) * (side_a - 1) + j - 1
                        self.copy(c, source, peer(0, j, c), slot).start()

                self.across(c, i, 0)

        def collect(self, c):
            for j in second_peers:
                self.copy(c, peer(0, -j, c), partner, 0).wait_recv()
                self.across(c, 0, j)
            for i in first_peers:
                for j in second_peers:
                    self.copy(c, peer(-i, -j, c), partner, 0).wait_recv()
                    self.across(c, i, j)

        def arrive(self, c):
            for i in range(side_b):
                for j in range(side_a):
                    self.copy(c, peer(i, j, c) + 1 - 2 * core, partner, 0).wait_recv()

        def finish(self, c):
            for slot in range(plane_slots(side_a, side_b)):
                self.copy(c, me, partner, slot).wait_send()

    ag_tile = width // ag_chunks
    rs_tile = width // rs_chunks
    first = Plane(tokens_all, rows, ag_tile, ag_send, ag_recv, lambda c: c < ag_routed)
    second = Plane(returned, cap, rs_tile, eo_send, eo_recv, lambda c: c >= rs_chunks - eo_routed)

    loads[0].wait()
    pl.semaphore_wait(barrier, len(greeted) + 1 + neighbours)

    for c in range(min(ahead, ag_chunks)):
        first.start(c)

    for load in loads[1:5]:
        load.wait()

    lanes = 128
    for j in range(width // lanes):
        cols = pl.ds(j * lanes, lanes)
        gain[0:1, cols] = gain16[j:j + 1, :].astype(F32)
        final_gain[0:1, cols] = final16[j:j + 1, :].astype(F32)

    chosen = picks[pl.ds(me, 1), :].astype(F32)
    column = jnp.broadcast_to(chosen, (cap, cap)).T
    for j in range(group // cap):
        at = lax.broadcasted_iota(jnp.int32, (cap, cap), 1).astype(F32) + float(j * cap)
        pick_map[:, pl.ds(j * cap, cap)] = jnp.where(column == at, 1.0, 0.0).astype(BF16)

    four = n == 4
    half = ag_chunks // 2
    step = jnp.where(2 * p < n, 1, -1)
    inner = (p > 0) & (p < n - 1)
    way_far = jnp.where(2 * p < n, 0, 1)
    way_end = 1 - way_far

    def z_copy(g, c, way, target):
        piece = gathered.at[g, :, span(c, ag_tile)]
        return pltpu.make_async_remote_copy(
            src_ref=piece,
            dst_ref=piece,
            send_sem=z_send.at[way, g, c],
            recv_sem=z_recv.at[g, c],
            device_id={"dp": target},
            device_id_type=MESH,
        )

    def rs_copy(g, c, slot, target):
        return pltpu.make_async_remote_copy(
            src_ref=part.at[g, :, span(c, rs_tile)],
            dst_ref=sums.at[slot, :, span(c, rs_tile)],
            send_sem=rs_send.at[g, c],
            recv_sem=rs_recv.at[slot, c],
            device_id={"dp": target},
            device_id_type=MESH,
        )

    def rs_start(g, c):
        @pl.when(g < p)
        def _():
            rs_copy(g, c, g, p - 1).start()

        @pl.when(g > p)
        def _():
            rs_copy(g, c, jnp.where(g == p + 1, n, g), p + 1).start()

    @pl.loop(0, ag_chunks + 2)
    def _(s):
        @pl.when(s < ag_chunks)
        def _():
            first.relay(s)

        @pl.when(s + ahead < ag_chunks)
        def _():
            first.start(s + ahead)

        @pl.when((s >= 1) & (s <= ag_chunks))
        def _():
            first.collect(s - 1)

        @pl.when(s >= 2)
        def _():
            c = s - 2
            cols = span(c, ag_tile)
            first.arrive(c)
            gathered[p, :, cols] = jnp.dot(
                pick_map[...], tokens_all[:, cols], preferred_element_type=F32
            ).astype(BF16)

            if four:
                @pl.when(inner)
                def _():
                    z_copy(p, c, way_end, p - step).start()

                @pl.when(jnp.logical_not(inner) | (c < half))
                def _():
                    z_copy(p, c, way_far, p + step).start()
            else:
                @pl.when(p < n - 1)
                def _():
                    z_copy(p, c, 0, p + 1).start()

                @pl.when(p > 0)
                def _():
                    z_copy(p, c, 1, p - 1).start()

    map_rows = min(group, 512) if keep_map else 256

    def build_map(i):
        at = lax.broadcasted_iota(jnp.int32, (map_rows, cap), 0) + i * map_rows
        return jnp.concatenate(
            [jnp.where(picks[e:e + 1, :] == at, 1.0, 0.0).astype(BF16) for e in range(experts)], axis=1
        )

    if keep_map:
        @pl.loop(0, group // map_rows)
        def _(i):
            out_map[span(i, map_rows)] = build_map(i)

    kv_acc[...] = jnp.zeros_like(kv_acc)
    squares[...] = jnp.zeros_like(squares)

    @pl.when(p == 0)
    def _():
        sums[n] = jnp.zeros(sums.shape[1:], BF16)

    @pl.when(p == n - 1)
    def _():
        sums[p] = jnp.zeros(sums.shape[1:], BF16)

    for load in loads[5:]:
        load.wait()

    ff_tile = ff // ff_steps

    def absorb(g, c, slot):
        cols = pl.ds(c * ag_tile, ag_tile)
        value = gathered[g, :, cols].astype(F32)
        squared = value * value
        total = squared[:, 0:lanes]
        for j in range(1, ag_tile // lanes):
            total = total + squared[:, j * lanes:(j + 1) * lanes]
        if c > 0:
            total = total + row_squares[slot]
        row_squares[slot] = total
        feed[...] = (value * gain[0:1, cols]).astype(BF16)
        closes = c == ag_chunks - 1
        if closes:
            row_scale[slot] = jnp.broadcast_to(
                lax.rsqrt(jnp.sum(total, axis=1, keepdims=True) * (1.0 / width) + 1e-06), total.shape
            )

        @pl.loop(0, ff // ff_tile)
        def _(i):
            tile = span(i, ff_tile)
            block = feed[...]
            gate = jnp.dot(block, gate_w[cols, tile], preferred_element_type=F32)
            up = jnp.dot(block, up_w[cols, tile], preferred_element_type=F32)
            if c > 0:
                gate = gate + gate_acc[slot, :, tile]
                up = up + up_acc[slot, :, tile]
            if closes:
                scale = row_scale[slot, :, 0:1]
                hidden[:, tile] = (jax.nn.gelu(gate * scale, approximate=True) * (up * scale)).astype(BF16)
            else:
                gate_acc[slot, :, tile] = gate
                up_acc[slot, :, tile] = up

    def emit(g):
        leads = ((g < p) & (p == n - 1)) | ((g > p) & (p == 0))
        wide = rs_tile * emit_group

        @pl.loop(0, rs_chunks // emit_group)
        def _(i):
            cols = span(i, wide)
            part[g, :, cols] = jnp.dot(
                hidden[...], down_w[:, cols], preferred_element_type=F32
            ).astype(BF16)

            @pl.when(leads)
            def _():
                for j in range(emit_group):
                    rs_start(g, i * emit_group + j)

    def forward(g, c):
        cols = span(c, rs_tile)
        rs_copy(g, c, g, p).wait_recv()
        part[g, :, cols] = (part[g, :, cols].astype(F32) + sums[g, :, cols].astype(F32)).astype(BF16)
        rs_start(g, c)

    leftmost = jnp.where(2 * p >= n - 1, 1, 0)
    closing = jnp.maximum(p, n - 1 - p)

    def flow(t, s):
        for turn in range(2):
            c = s - turn * lag
            to_left = leftmost if turn == 0 else 1 - leftmost
            g = jnp.where(to_left == 1, n - 1 - t, t)
            live = jnp.where(to_left == 1, (g < p) & (p < n - 1), (g > p) & (p > 0))

            @pl.when(live & (c >= 0) & (c < rs_chunks))
            def _():
                forward(g, c)

    def final(c):
        cols = span(c, rs_tile)

        @pl.when(p < n - 1)
        def _():
            rs_copy(p, c, p, p).wait_recv()

        @pl.when(p > 0)
        def _():
            rs_copy(p, c, n, p).wait_recv()

        value = (
            part[p, :, cols].astype(F32) + sums[p, :, cols].astype(F32) + sums[n, :, cols].astype(F32)
        )

        returned[span(me, cap), cols] = (value * prob[:, 0:1]).astype(BF16)
        second.start(c)

    logits = jnp.zeros((cap, experts), F32)
    for c in range(ag_chunks):
        absorb(p, c, 0)
        logits = logits + lax.dot_general(
            feed[...], router[:, pl.ds(c * ag_tile, ag_tile)], (((1,), (1,)), ((), ())), preferred_element_type=F32
        )
    emit(p)
    logits = logits * row_scale[0, :, 0:1]
    mine = lax.broadcasted_iota(jnp.int32, logits.shape, 1) == me
    chance = jnp.sum(jnp.where(mine, jax.nn.sigmoid(logits), 0.0), axis=1, keepdims=True)
    prob[...] = jnp.broadcast_to(chance, prob.shape)

    def take(g, c):
        z_copy(g, c, 0, p).wait_recv()

    if four:
        @pl.when(jnp.logical_not(inner))
        def _():
            @pl.loop(0, n - 1)
            def _(j):
                g = p + step * jnp.where(j == 0, 1, n - 1 - (j - 1))
                for c in range(ag_chunks):
                    take(g, c)
                    absorb(g, c, 0)
                emit(g)

        @pl.when(inner)
        def _():
            edge, mate, far = p - step, p + step, p + 2 * step
            for c in range(ag_chunks):
                take(edge, c)
                z_copy(edge, c, way_far, mate).start()
                if c == ag_chunks - 1:
                    for k in range(half, ag_chunks):
                        z_copy(p, k, way_far, mate).start()
                if c >= half:
                    take(far, c - half)
                    z_copy(far, c - half, way_end, edge).start()
                absorb(edge, c, 0)
                if c == ag_chunks - 1:
                    emit(edge)
                if c >= half:
                    absorb(far, c - half, 1)
                else:
                    take(mate, c)
                    absorb(mate, c, 2)
            for c in range(ag_chunks - half, ag_chunks):
                take(far, c)
                z_copy(far, c, way_end, edge).start()
                if c == ag_chunks - 1:
                    for k in range(half):
                        z_copy(mate, k, way_end, edge).start()
                absorb(far, c, 1)
            emit(far)
            for c in range(half, ag_chunks):
                take(mate, c)
                z_copy(mate, c, way_end, edge).start()
                absorb(mate, c, 2)
            emit(mate)

            @pl.loop(0, rs_chunks + lag)
            def _(s):
                @pl.when(s < rs_chunks)
                def _():
                    forward(far, s)

                @pl.when(s >= lag)
                def _():
                    forward(edge, s - lag)
    else:
        def side_group(t, side):
            return p + t * (2 * side - 1)

        @pl.loop(1, n)
        def _(t):
            for c in range(ag_chunks):
                for side in range(2):
                    g = side_group(t, side)

                    @pl.when((g >= 0) & (g < n))
                    def _():
                        z_copy(g, c, 0, p).wait_recv()
                        onward = p + 1 - 2 * side

                        @pl.when((onward >= 0) & (onward < n))
                        def _():
                            z_copy(g, c, side, onward).start()

                        absorb(g, c, side)
                        if c == ag_chunks - 1:
                            emit(g)

            @pl.when(t < n - 1)
            def _():
                @pl.loop(0, rs_chunks + lag)
                def _(s):
                    flow(t, s)

                    @pl.when((t == closing) & (s >= lag))
                    def _():
                        final(s - lag)

    @pl.loop(0, ag_chunks)
    def _(c):
        first.finish(c)

        @pl.loop(0, n)
        def _(g):
            @pl.when((g <= p) & (p < n - 1))
            def _():
                z_copy(g, c, 0, p).wait_send()

            @pl.when((g >= p) & (p > 0))
            def _():
                z_copy(g, c, 1, p).wait_send()

    def consume(c):
        cols = span(c, rs_tile)
        second.arrive(c)

        @pl.loop(0, group // map_rows)
        def _(i):
            piece = span(i, map_rows)
            chosen_map = out_map[piece] if keep_map else build_map(i)
            value = (
                tokens_all[piece, cols].astype(F32)
                + jnp.dot(chosen_map, returned[:, cols], preferred_element_type=F32)
            ).astype(BF16)
            tokens_all[piece, cols] = value
            wide = value.astype(F32)
            square_sum = wide * wide
            total = square_sum[:, 0:lanes]
            for j in range(1, rs_tile // lanes):
                total = total + square_sum[:, j * lanes:(j + 1) * lanes]
            squares[piece] += total
            scaled = (wide * final_gain[0:1, cols]).astype(BF16)
            kv_acc[:, piece] += lax.dot_general(
                kv_w[:, cols], scaled, (((1,), (1,)), ((), ())), preferred_element_type=F32
            )

    at_relay, at_collect, at_consume = depth

    after = lag if four else 0

    @pl.loop(0, rs_chunks + at_consume + after)
    def _(s):
        if four:
            @pl.when(inner & (s < rs_chunks))
            def _():
                forward(p + step, s)
        else:
            flow(n - 1, s)

        c = s - after

        @pl.when((c >= 0) & (c < rs_chunks) & (four | (closing == n - 1)))
        def _():
            final(c)

        @pl.when((c >= at_relay) & (c < rs_chunks + at_relay))
        def _():
            second.relay(c - at_relay)

        @pl.when((c >= at_collect) & (c < rs_chunks + at_collect))
        def _():
            second.collect(c - at_collect)

        @pl.when(c >= at_consume)
        def _():
            consume(c - at_consume)

    moe_store = pltpu.make_async_copy(tokens_all.at[own], moe_out, out_sem.at[0])
    moe_store.start()
    mean = jnp.sum(squares[...].T, axis=0, keepdims=True) * (1.0 / width)
    scale = lax.rsqrt(mean + 1e-06)
    out_rows = 128
    stores = []
    for i in range(heads // out_rows):
        piece = pl.ds(i * out_rows, out_rows)
        kv_stage[piece] = (kv_acc[piece] * scale).astype(BF16)
        store = pltpu.make_async_copy(kv_stage.at[piece], kv_out.at[piece], out_sem.at[1 + i])
        store.start()
        stores.append(store)

    @pl.loop(0, rs_chunks)
    def _(c):
        second.finish(c)

    @pl.loop(0, n)
    def _(g):
        @pl.when(g != p)
        def _():
            @pl.loop(0, rs_chunks)
            def _(c):
                rs_copy(g, c, g, p).wait_send()

    moe_store.wait()
    for store in stores:
        store.wait()


def local(
    tokens,
    norm_gain,
    router_weight,
    gate_weight,
    up_weight,
    down_weight,
    expert_picks,
    final_gain,
    kv_weight,
):
    n = lax.axis_size("dp")
    experts = lax.axis_size("expert")
    rows, width = tokens.shape
    ff = gate_weight.shape[2]
    cap = expert_picks.shape[2]
    group = experts * rows
    chips = experts // 2
    side_a = max(d for d in range(1, math.isqrt(chips) + 1) if chips % d == 0)
    side_b = chips // side_a
    kv_matrix = kv_weight.reshape(width, -1).T
    heads = kv_matrix.shape[0]
    ag_chunks = 4
    rs_chunks = 8
    ahead = 2
    ag_routed = 0
    eo_routed = 0
    lag = 2
    depth = (2, 4, 5)
    ff_steps = 1
    emit_group = 4
    keep_map = group * experts * cap * 2 <= 4 * 1024 * 1024
    dma = pltpu.SemaphoreType.DMA
    slots = plane_slots(side_a, side_b)
    hbm = pl.BlockSpec(memory_space=pl.ANY)
    moe_out, kv_rows = pl.pallas_call(
        functools.partial(kernel, n, experts, side_a, side_b, ag_chunks, rs_chunks, ahead, ag_routed, eo_routed, lag, depth, ff_steps, emit_group, keep_map),
        out_shape=(
            jax.ShapeDtypeStruct((rows, width), BF16),
            jax.ShapeDtypeStruct((heads, group), BF16),
        ),
        in_specs=[hbm] * 9,
        out_specs=(hbm, hbm),
        scratch_shapes=[
            pltpu.VMEM((width, ff), BF16),
            pltpu.VMEM((width, ff), BF16),
            pltpu.VMEM((ff, width), BF16),
            pltpu.VMEM((heads, width), BF16),
            pltpu.VMEM((group, width), BF16),
            pltpu.VMEM((n, cap, width), BF16),
            pltpu.VMEM((cap, width // ag_chunks), BF16),
            pltpu.VMEM((3, cap, ff), F32),
            pltpu.VMEM((3, cap, ff), F32),
            pltpu.VMEM((3, cap, 128), F32),
            pltpu.VMEM((3, cap, 128), F32),
            pltpu.VMEM((cap, ff), BF16),
            pltpu.VMEM((n, cap, width), BF16),
            pltpu.VMEM((n + 1, cap, width), BF16),
            pltpu.VMEM((experts * cap, width), BF16),
            pltpu.VMEM((width // 128, 128), BF16),
            pltpu.VMEM((width // 128, 128), BF16),
            pltpu.VMEM((1, width), F32),
            pltpu.VMEM((1, width), F32),
            pltpu.VMEM((experts, width), BF16),
            pltpu.VMEM((experts, cap), jnp.int32),
            pltpu.VMEM((cap, group), BF16),
            pltpu.VMEM((group, experts * cap) if keep_map else (8, 128), BF16),
            pltpu.VMEM((cap, 128), F32),
            pltpu.VMEM((group, 128), F32),
            pltpu.VMEM((heads, group), F32),
            pltpu.VMEM((heads, group), BF16),
            dma((9,)),
            dma((slots, ag_chunks)),
            dma((experts, ag_chunks)),
            dma((2, n, ag_chunks)),
            dma((n, ag_chunks)),
            dma((n, rs_chunks)),
            dma((n + 1, rs_chunks)),
            dma((slots, rs_chunks)),
            dma((experts, rs_chunks)),
            dma((1 + heads // 128,)),
        ],
        compiler_params=pltpu.CompilerParams(
            collective_id=0, has_side_effects=True, vmem_limit_bytes=67043328
        ),
    )(
        tokens, norm_gain.reshape(-1, 128), router_weight.T, gate_weight, up_weight, down_weight,
        expert_picks[0], final_gain.reshape(-1, 128), kv_matrix,
    )
    kv_cache = kv_rows.T.reshape((group,) + kv_weight.shape[1:])
    return (moe_out, kv_cache)


def solution(mesh):
    in_specs = (
        P(("dp", "expert"), None),
        P(),
        P(),
        P("expert", None, "dp"),
        P("expert", None, "dp"),
        P("expert", "dp", None),
        P("dp", None, None),
        P(),
        P(None, "expert", None, None, None),
    )
    out_specs = (P(("dp", "expert"), None), P("dp", "expert", None, None, None))
    return jax.shard_map(local, mesh=mesh, in_specs=in_specs, out_specs=out_specs, check_vma=False)
```

```python
import functools
import math

import jax
import jax.numpy as jnp
from jax import lax
from jax.experimental import pallas as pl
from jax.experimental.pallas import tpu as pltpu
from jax.sharding import PartitionSpec as P

MESH = pl.DeviceIdType.MESH
F32 = jnp.float32
BF16 = jnp.bfloat16


def plane_slots(side_a, side_b):
    return (side_a - 1) + (side_b - 1) + 1 + (side_a - 1) * (side_b - 1) + side_a * side_b - 1


def kernel(
    n, experts, side_a, side_b, ag_chunks, rs_chunks, ahead, ag_routed, eo_routed, lag, depth, ff_steps, emit_group, keep_map,
    tokens_hbm, gain_hbm, router_hbm, gate_hbm, up_hbm, down_hbm, picks_hbm, final_gain_hbm, kv_hbm,
    moe_out, kv_out,
    gate_w, up_w, down_w, kv_w, tokens_all, gathered, feed, gate_acc, up_acc, row_squares, row_scale, hidden, part, sums, returned,
    gain16, final16, gain, final_gain, router, picks, pick_map, out_map, prob, squares, kv_acc, kv_stage,
    load_sem, ag_send, ag_recv, z_send, z_recv, rs_send, rs_recv, eo_send, eo_recv, out_sem,
):
    p = lax.axis_index("dp")
    me = lax.axis_index("expert")
    cap = picks.shape[1]
    group, width = tokens_all.shape
    rows = group // experts
    ff = gate_w.shape[1]
    heads = kv_acc.shape[0]
    core = lax.rem(me, 2)
    chip = lax.div(me, 2)
    row_at = lax.div(chip, side_b)
    col_at = lax.rem(chip, side_b)
    partner = chip * 2 + (1 - core)

    def span(index, size):
        return pl.ds(pl.multiple_of(index * size, size), size)

    own = span(me, rows)
    loads = [
        pltpu.make_async_copy(src, dst, load_sem.at[i])
        for i, (src, dst) in enumerate((
            (tokens_hbm, tokens_all.at[own]),
            (picks_hbm, picks),
            (gain_hbm, gain16),
            (final_gain_hbm, final16),
            (router_hbm, router),
            (gate_hbm.at[0], gate_w),
            (up_hbm.at[0], up_w),
            (down_hbm.at[0], down_w),
            (kv_hbm, kv_w),
        ))
    ]
    for load in loads:
        load.start()

    def place(a, b):
        return (lax.rem(a + side_a, side_a) * side_b + lax.rem(b + side_b, side_b)) * 2 + core

    square = side_a == side_b

    def peer(i, j, c):
        straight = place(row_at + j, col_at + i)
        if not square:
            return straight
        return jnp.where(lax.rem(c, 2) == 0, straight, place(row_at + i, col_at + j))

    barrier = pltpu.get_barrier_semaphore()

    def greet(target):
        pl.semaphore_signal(barrier, inc=1, device_id={"expert": target}, device_id_type=MESH)

    greeted = [
        (j, i) for j in range(side_a) for i in range(side_b)
        if (i > 0 or j > 0) and (i == 0 or j == 0 or ag_routed + eo_routed > 0)
    ]
    for j, i in greeted:
        greet(place(row_at + j, col_at + i))
    greet(partner)

    @pl.when(p > 0)
    def _():
        pl.semaphore_signal(barrier, inc=1, device_id={"dp": p - 1}, device_id_type=MESH)

    @pl.when(p < n - 1)
    def _():
        pl.semaphore_signal(barrier, inc=1, device_id={"dp": p + 1}, device_id_type=MESH)

    neighbours = jnp.where(p > 0, 1, 0) + jnp.where(p < n - 1, 1, 0)
    first_peers = range(1, side_b)
    second_peers = range(1, side_a)
    direct = side_a + side_b - 2

    class Plane:
        def __init__(self, full, unit, tile, send, recv, routed):
            self.full, self.unit, self.tile, self.send, self.recv = full, unit, tile, send, recv
            self.routed = routed

        def copy(self, c, source, target, slot):
            where = self.full.at[span(source, self.unit), span(c, self.tile)]
            return pltpu.make_async_remote_copy(
                src_ref=where,
                dst_ref=where,
                send_sem=self.send.at[slot, c],
                recv_sem=self.recv.at[source, c],
                device_id={"expert": target},
                device_id_type=MESH,
            )

        def start(self, c):
            for i in first_peers:
                self.copy(c, me, peer(i, 0, c), i - 1).start()
            for j in second_peers:
                self.copy(c, me, peer(0, j, c), side_b - 1 + j - 1).start()
            self.copy(c, me, partner, direct).start()

            @pl.when(self.routed(c))
            def _():
                for i in first_peers:
                    for j in second_peers:
                        self.copy(c, me, peer(i, j, c), direct + 1 + (i - 1) * (side_a - 1) + j - 1).start()

        def across(self, c, i, j):
            source = peer(-i, -j, c)
            slot = direct + 1 + (side_a - 1) * (side_b - 1) + i * side_a + j - 1
            piece = self.copy(c, source, partner, slot)
            piece.start()

        def relay(self, c):
            for i in first_peers:
                source = peer(-i, 0, c)
                self.copy(c, source, partner, 0).wait_recv()

                @pl.when(jnp.logical_not(self.routed(c)))
                def _():
                    for j in second_peers:
                        slot = direct + 1 + (i - 1) * (side_a - 1) + j - 1
                        self.copy(c, source, peer(0, j, c), slot).start()

                self.across(c, i, 0)

        def collect(self, c):
            for j in second_peers:
                self.copy(c, peer(0, -j, c), partner, 0).wait_recv()
                self.across(c, 0, j)
            for i in first_peers:
                for j in second_peers:
                    self.copy(c, peer(-i, -j, c), partner, 0).wait_recv()
                    self.across(c, i, j)

        def arrive(self, c):
            for i in range(side_b):
                for j in range(side_a):
                    self.copy(c, peer(i, j, c) + 1 - 2 * core, partner, 0).wait_recv()

        def finish(self, c):
            for slot in range(plane_slots(side_a, side_b)):
                self.copy(c, me, partner, slot).wait_send()

    ag_tile = width // ag_chunks
    rs_tile = width // rs_chunks
    first = Plane(tokens_all, rows, ag_tile, ag_send, ag_recv, lambda c: c < ag_routed)
    second = Plane(returned, cap, rs_tile, eo_send, eo_recv, lambda c: c >= rs_chunks - eo_routed)

    loads[0].wait()
    pl.semaphore_wait(barrier, len(greeted) + 1 + neighbours)

    for c in range(min(ahead, ag_chunks)):
        first.start(c)

    for load in loads[1:5]:
        load.wait()

    lanes = 128
    for j in range(width // lanes):
        cols = pl.ds(j * lanes, lanes)
        gain[0:1, cols] = gain16[j:j + 1, :].astype(F32)
        final_gain[0:1, cols] = final16[j:j + 1, :].astype(F32)

    chosen = picks[pl.ds(me, 1), :].astype(F32)
    column = jnp.broadcast_to(chosen, (cap, cap)).T
    for j in range(group // cap):
        at = lax.broadcasted_iota(jnp.int32, (cap, cap), 1).astype(F32) + float(j * cap)
        pick_map[:, pl.ds(j * cap, cap)] = jnp.where(column == at, 1.0, 0.0).astype(BF16)

    four = n == 4
    half = ag_chunks // 2
    step = jnp.where(2 * p < n, 1, -1)
    inner = (p > 0) & (p < n - 1)
    way_far = jnp.where(2 * p < n, 0, 1)
    way_end = 1 - way_far

    def z_copy(g, c, way, target):
        piece = gathered.at[g, :, span(c, ag_tile)]
        return pltpu.make_async_remote_copy(
            src_ref=piece,
            dst_ref=piece,
            send_sem=z_send.at[way, g, c],
            recv_sem=z_recv.at[g, c],
            device_id={"dp": target},
            device_id_type=MESH,
        )

    def rs_copy(g, c, slot, target):
        return pltpu.make_async_remote_copy(
            src_ref=part.at[g, :, span(c, rs_tile)],
            dst_ref=sums.at[slot, :, span(c, rs_tile)],
            send_sem=rs_send.at[g, c],
            recv_sem=rs_recv.at[slot, c],
            device_id={"dp": target},
            device_id_type=MESH,
        )

    def rs_start(g, c):
        @pl.when(g < p)
        def _():
            rs_copy(g, c, g, p - 1).start()

        @pl.when(g > p)
        def _():
            rs_copy(g, c, jnp.where(g == p + 1, n, g), p + 1).start()

    @pl.loop(0, ag_chunks + 2)
    def _(s):
        @pl.when(s < ag_chunks)
        def _():
            first.relay(s)

        @pl.when(s + ahead < ag_chunks)
        def _():
            first.start(s + ahead)

        @pl.when((s >= 1) & (s <= ag_chunks))
        def _():
            first.collect(s - 1)

        @pl.when(s >= 2)
        def _():
            c = s - 2
            cols = span(c, ag_tile)
            first.arrive(c)
            gathered[p, :, cols] = jnp.dot(
                pick_map[...], tokens_all[:, cols], preferred_element_type=F32
            ).astype(BF16)

            if four:
                @pl.when(inner)
                def _():
                    z_copy(p, c, way_end, p - step).start()

                @pl.when(jnp.logical_not(inner) | (c < half))
                def _():
                    z_copy(p, c, way_far, p + step).start()
            else:
                @pl.when(p < n - 1)
                def _():
                    z_copy(p, c, 0, p + 1).start()

                @pl.when(p > 0)
                def _():
                    z_copy(p, c, 1, p - 1).start()

    map_rows = min(group, 512) if keep_map else 256

    def build_map(i):
        at = lax.broadcasted_iota(jnp.int32, (map_rows, cap), 0) + i * map_rows
        return jnp.concatenate(
            [jnp.where(picks[e:e + 1, :] == at, 1.0, 0.0).astype(BF16) for e in range(experts)], axis=1
        )

    if keep_map:
        @pl.loop(0, group // map_rows)
        def _(i):
            out_map[span(i, map_rows)] = build_map(i)

    kv_acc[...] = jnp.zeros_like(kv_acc)
    squares[...] = jnp.zeros_like(squares)

    @pl.when(p == 0)
    def _():
        sums[n] = jnp.zeros(sums.shape[1:], BF16)

    @pl.when(p == n - 1)
    def _():
        sums[p] = jnp.zeros(sums.shape[1:], BF16)

    for load in loads[5:]:
        load.wait()

    ff_tile = ff // ff_steps

    def absorb(g, c, slot):
        cols = pl.ds(c * ag_tile, ag_tile)
        value = gathered[g, :, cols].astype(F32)
        squared = value * value
        total = squared[:, 0:lanes]
        for j in range(1, ag_tile // lanes):
            total = total + squared[:, j * lanes:(j + 1) * lanes]
        if c > 0:
            total = total + row_squares[slot]
        row_squares[slot] = total
        feed[...] = (value * gain[0:1, cols]).astype(BF16)
        closes = c == ag_chunks - 1
        if closes:
            row_scale[slot] = jnp.broadcast_to(
                lax.rsqrt(jnp.sum(total, axis=1, keepdims=True) * (1.0 / width) + 1e-06), total.shape
            )

        @pl.loop(0, ff // ff_tile)
        def _(i):
            tile = span(i, ff_tile)
            block = feed[...]
            gate = jnp.dot(block, gate_w[cols, tile], preferred_element_type=F32)
            up = jnp.dot(block, up_w[cols, tile], preferred_element_type=F32)
            if c > 0:
                gate = gate + gate_acc[slot, :, tile]
                up = up + up_acc[slot, :, tile]
            if closes:
                scale = row_scale[slot, :, 0:1]
                hidden[:, tile] = (jax.nn.gelu(gate * scale, approximate=True) * (up * scale)).astype(BF16)
            else:
                gate_acc[slot, :, tile] = gate
                up_acc[slot, :, tile] = up

    def emit(g):
        leads = ((g < p) & (p == n - 1)) | ((g > p) & (p == 0))
        wide = rs_tile * emit_group

        @pl.loop(0, rs_chunks // emit_group)
        def _(i):
            cols = span(i, wide)
            part[g, :, cols] = jnp.dot(
                hidden[...], down_w[:, cols], preferred_element_type=F32
            ).astype(BF16)

            @pl.when(leads)
            def _():
                for j in range(emit_group):
                    rs_start(g, i * emit_group + j)

    def forward(g, c):
        cols = span(c, rs_tile)
        rs_copy(g, c, g, p).wait_recv()
        part[g, :, cols] = (part[g, :, cols].astype(F32) + sums[g, :, cols].astype(F32)).astype(BF16)
        rs_start(g, c)

    leftmost = jnp.where(2 * p >= n - 1, 1, 0)
    closing = jnp.maximum(p, n - 1 - p)

    def flow(t, s):
        for turn in range(2):
            c = s - turn * lag
            to_left = leftmost if turn == 0 else 1 - leftmost
            g = jnp.where(to_left == 1, n - 1 - t, t)
            live = jnp.where(to_left == 1, (g < p) & (p < n - 1), (g > p) & (p > 0))

            @pl.when(live & (c >= 0) & (c < rs_chunks))
            def _():
                forward(g, c)

    def final(c):
        cols = span(c, rs_tile)

        @pl.when(p < n - 1)
        def _():
            rs_copy(p, c, p, p).wait_recv()

        @pl.when(p > 0)
        def _():
            rs_copy(p, c, n, p).wait_recv()

        value = (
            part[p, :, cols].astype(F32) + sums[p, :, cols].astype(F32) + sums[n, :, cols].astype(F32)
        )

        returned[span(me, cap), cols] = (value * prob[:, 0:1]).astype(BF16)
        second.start(c)

    logits = jnp.zeros((cap, experts), F32)
    for c in range(ag_chunks):
        absorb(p, c, 0)
        logits = logits + lax.dot_general(
            feed[...], router[:, pl.ds(c * ag_tile, ag_tile)], (((1,), (1,)), ((), ())), preferred_element_type=F32
        )
    emit(p)
    logits = logits * row_scale[0, :, 0:1]
    mine = lax.broadcasted_iota(jnp.int32, logits.shape, 1) == me
    chance = jnp.sum(jnp.where(mine, jax.nn.sigmoid(logits), 0.0), axis=1, keepdims=True)
    prob[...] = jnp.broadcast_to(chance, prob.shape)

    def take(g, c):
        z_copy(g, c, 0, p).wait_recv()

    if four:
        @pl.when(jnp.logical_not(inner))
        def _():
            @pl.loop(0, n - 1)
            def _(j):
                g = p + step * jnp.where(j == 0, 1, n - 1 - (j - 1))
                for c in range(ag_chunks):
                    take(g, c)
                    absorb(g, c, 0)
                emit(g)

        @pl.when(inner)
        def _():
            edge, mate, far = p - step, p + step, p + 2 * step
            for c in range(ag_chunks):
                take(edge, c)
                z_copy(edge, c, way_far, mate).start()
                if c == ag_chunks - 1:
                    for k in range(half, ag_chunks):
                        z_copy(p, k, way_far, mate).start()
                if c >= half:
                    take(far, c - half)
                    z_copy(far, c - half, way_end, edge).start()
                absorb(edge, c, 0)
                if c == ag_chunks - 1:
                    emit(edge)
                if c >= half:
                    absorb(far, c - half, 1)
                else:
                    take(mate, c)
                    absorb(mate, c, 2)
            for c in range(ag_chunks - half, ag_chunks):
                take(far, c)
                z_copy(far, c, way_end, edge).start()
                if c == ag_chunks - 1:
                    for k in range(half):
                        z_copy(mate, k, way_end, edge).start()
                absorb(far, c, 1)
            emit(far)
            for c in range(half, ag_chunks):
                take(mate, c)
                z_copy(mate, c, way_end, edge).start()
                absorb(mate, c, 2)
            emit(mate)

            @pl.loop(0, rs_chunks + lag)
            def _(s):
                @pl.when(s < rs_chunks)
                def _():
                    forward(far, s)

                @pl.when(s >= lag)
                def _():
                    forward(edge, s - lag)
    else:
        def side_group(t, side):
            return p + t * (2 * side - 1)

        @pl.loop(1, n)
        def _(t):
            for c in range(ag_chunks):
                for side in range(2):
                    g = side_group(t, side)

                    @pl.when((g >= 0) & (g < n))
                    def _():
                        z_copy(g, c, 0, p).wait_recv()
                        onward = p + 1 - 2 * side

                        @pl.when((onward >= 0) & (onward < n))
                        def _():
                            z_copy(g, c, side, onward).start()

                        absorb(g, c, side)
                        if c == ag_chunks - 1:
                            emit(g)

            @pl.when(t < n - 1)
            def _():
                @pl.loop(0, rs_chunks + lag)
                def _(s):
                    flow(t, s)

                    @pl.when((t == closing) & (s >= lag))
                    def _():
                        final(s - lag)

    @pl.loop(0, ag_chunks)
    def _(c):
        first.finish(c)

        @pl.loop(0, n)
        def _(g):
            @pl.when((g <= p) & (p < n - 1))
            def _():
                z_copy(g, c, 0, p).wait_send()

            @pl.when((g >= p) & (p > 0))
            def _():
                z_copy(g, c, 1, p).wait_send()

    def consume(c):
        cols = span(c, rs_tile)
        second.arrive(c)

        @pl.loop(0, group // map_rows)
        def _(i):
            piece = span(i, map_rows)
            chosen_map = out_map[piece] if keep_map else build_map(i)
            value = (
                tokens_all[piece, cols].astype(F32)
                + jnp.dot(chosen_map, returned[:, cols], preferred_element_type=F32)
            ).astype(BF16)
            tokens_all[piece, cols] = value
            wide = value.astype(F32)
            square_sum = wide * wide
            total = square_sum[:, 0:lanes]
            for j in range(1, rs_tile // lanes):
                total = total + square_sum[:, j * lanes:(j + 1) * lanes]
            squares[piece] += total
            scaled = (wide * final_gain[0:1, cols]).astype(BF16)
            kv_acc[:, piece] += lax.dot_general(
                kv_w[:, cols], scaled, (((1,), (1,)), ((), ())), preferred_element_type=F32
            )

    at_relay, at_collect, at_consume = depth

    after = lag if four else 0

    @pl.loop(0, rs_chunks + at_consume + after)
    def _(s):
        if four:
            @pl.when(inner & (s < rs_chunks))
            def _():
                forward(p + step, s)
        else:
            flow(n - 1, s)

        c = s - after

        @pl.when((c >= 0) & (c < rs_chunks) & (four | (closing == n - 1)))
        def _():
            final(c)

        @pl.when((c >= at_relay) & (c < rs_chunks + at_relay))
        def _():
            second.relay(c - at_relay)

        @pl.when((c >= at_collect) & (c < rs_chunks + at_collect))
        def _():
            second.collect(c - at_collect)

        @pl.when(c >= at_consume)
        def _():
            consume(c - at_consume)

    moe_store = pltpu.make_async_copy(tokens_all.at[own], moe_out, out_sem.at[0])
    moe_store.start()
    mean = jnp.sum(squares[...].T, axis=0, keepdims=True) * (1.0 / width)
    scale = lax.rsqrt(mean + 1e-06)
    out_rows = 128
    stores = []
    for i in range(heads // out_rows):
        piece = pl.ds(i * out_rows, out_rows)
        kv_stage[piece] = (kv_acc[piece] * scale).astype(BF16)
        store = pltpu.make_async_copy(kv_stage.at[piece], kv_out.at[piece], out_sem.at[1 + i])
        store.start()
        stores.append(store)

    @pl.loop(0, rs_chunks)
    def _(c):
        second.finish(c)

    @pl.loop(0, n)
    def _(g):
        @pl.when(g != p)
        def _():
            @pl.loop(0, rs_chunks)
            def _(c):
                rs_copy(g, c, g, p).wait_send()

    moe_store.wait()
    for store in stores:
        store.wait()


def local(
    tokens,
    norm_gain,
    router_weight,
    gate_weight,
    up_weight,
    down_weight,
    expert_picks,
    final_gain,
    kv_weight,
):
    n = lax.axis_size("dp")
    experts = lax.axis_size("expert")
    rows, width = tokens.shape
    ff = gate_weight.shape[2]
    cap = expert_picks.shape[2]
    group = experts * rows
    chips = experts // 2
    side_a = max(d for d in range(1, math.isqrt(chips) + 1) if chips % d == 0)
    side_b = chips // side_a
    kv_matrix = kv_weight.reshape(width, -1).T
    heads = kv_matrix.shape[0]
    ag_chunks = 4
    rs_chunks = 8
    ahead = 2
    ag_routed = 0
    eo_routed = 0
    lag = 2
    depth = (2, 5, 7)
    ff_steps = 1
    emit_group = 4
    keep_map = group * experts * cap * 2 <= 4 * 1024 * 1024
    dma = pltpu.SemaphoreType.DMA
    slots = plane_slots(side_a, side_b)
    hbm = pl.BlockSpec(memory_space=pl.ANY)
    moe_out, kv_rows = pl.pallas_call(
        functools.partial(kernel, n, experts, side_a, side_b, ag_chunks, rs_chunks, ahead, ag_routed, eo_routed, lag, depth, ff_steps, emit_group, keep_map),
        out_shape=(
            jax.ShapeDtypeStruct((rows, width), BF16),
            jax.ShapeDtypeStruct((heads, group), BF16),
        ),
        in_specs=[hbm] * 9,
        out_specs=(hbm, hbm),
        scratch_shapes=[
            pltpu.VMEM((width, ff), BF16),
            pltpu.VMEM((width, ff), BF16),
            pltpu.VMEM((ff, width), BF16),
            pltpu.VMEM((heads, width), BF16),
            pltpu.VMEM((group, width), BF16),
            pltpu.VMEM((n, cap, width), BF16),
            pltpu.VMEM((cap, width // ag_chunks), BF16),
            pltpu.VMEM((3, cap, ff), F32),
            pltpu.VMEM((3, cap, ff), F32),
            pltpu.VMEM((3, cap, 128), F32),
            pltpu.VMEM((3, cap, 128), F32),
            pltpu.VMEM((cap, ff), BF16),
            pltpu.VMEM((n, cap, width), BF16),
            pltpu.VMEM((n + 1, cap, width), BF16),
            pltpu.VMEM((experts * cap, width), BF16),
            pltpu.VMEM((width // 128, 128), BF16),
            pltpu.VMEM((width // 128, 128), BF16),
            pltpu.VMEM((1, width), F32),
            pltpu.VMEM((1, width), F32),
            pltpu.VMEM((experts, width), BF16),
            pltpu.VMEM((experts, cap), jnp.int32),
            pltpu.VMEM((cap, group), BF16),
            pltpu.VMEM((group, experts * cap) if keep_map else (8, 128), BF16),
            pltpu.VMEM((cap, 128), F32),
            pltpu.VMEM((group, 128), F32),
            pltpu.VMEM((heads, group), F32),
            pltpu.VMEM((heads, group), BF16),
            dma((9,)),
            dma((slots, ag_chunks)),
            dma((experts, ag_chunks)),
            dma((2, n, ag_chunks)),
            dma((n, ag_chunks)),
            dma((n, rs_chunks)),
            dma((n + 1, rs_chunks)),
            dma((slots, rs_chunks)),
            dma((experts, rs_chunks)),
            dma((1 + heads // 128,)),
        ],
        compiler_params=pltpu.CompilerParams(
            collective_id=0, has_side_effects=True, vmem_limit_bytes=67043328
        ),
    )(
        tokens, norm_gain.reshape(-1, 128), router_weight.T, gate_weight, up_weight, down_weight,
        expert_picks[0], final_gain.reshape(-1, 128), kv_matrix,
    )
    kv_cache = kv_rows.T.reshape((group,) + kv_weight.shape[1:])
    return (moe_out, kv_cache)


def solution(mesh):
    in_specs = (
        P(("dp", "expert"), None),
        P(),
        P(),
        P("expert", None, "dp"),
        P("expert", None, "dp"),
        P("expert", "dp", None),
        P("dp", None, None),
        P(),
        P(None, "expert", None, None, None),
    )
    out_specs = (P(("dp", "expert"), None), P("dp", "expert", None, None, None))
    return jax.shard_map(local, mesh=mesh, in_specs=in_specs, out_specs=out_specs, check_vma=False)
```
